32 devices in a mesh: section: 4 (over y, x), ctx: 4 (over z), dp: 2 (over core).
Axes of the slice: x: 2, y: 2, z: 4, core: 2. Of those that a mesh axis runs over, the one named last changes fastest.
Arguments:
- first_input: bfloat16 [4, 2, 512, 2048], P('section', 'dp', 'ctx'), may hold values from -14 to 14
- second_input: bfloat16 [4, 2, 512, 2048], P('section', 'dp', 'ctx'), may hold values from -6 to 6
- upstream: bfloat16 [4, 2, 512, 2048], P('section', 'dp', 'ctx'), may hold values from -6 to 6
- first_picks: int32 [4, 2, 512, 6], P('section', 'dp', 'ctx'), may hold values from 0 to 63, all different within a row
- second_picks: int32 [4, 2, 512, 6], P('section', 'dp', 'ctx'), may hold values from 0 to 63, all different within a row
- gate_grads: float32 [4, 2, 512, 6], P('section', 'dp', 'ctx'), may hold values from -0.0009 to 0.0009
- norm_gain: float32 [4, 2048], P('section'), may hold values from 0.5 to 1.5
- router_weight: float32 [4, 64, 2048], P('section'), may hold values from -0.25 to 0.25
- gate_weight: bfloat16 [4, 2048, 1280], P('section', 'ctx'), may hold values from -0.125 to 0.125
- up_weight: bfloat16 [4, 2048, 1280], P('section', 'ctx'), may hold values from -0.125 to 0.125
- down_weight: bfloat16 [4, 1280, 2048], P('section', None, 'ctx'), may hold values from -0.15625 to 0.15625
Outputs:
- arrived: bfloat16 [4, 2, 512, 2048], P('section', 'dp', 'ctx')
- routing: float32 [4, 2, 512, 6], P('section', 'dp', 'ctx')
- input_grad: bfloat16 [4, 2, 512, 2048], P('section', 'dp', 'ctx')
- router_grad: float32 [4, 64, 2048], P('section')
- balance: float32 [4, 2, 2], P('section', 'dp')
The draws below stay inside these ranges and needn't reach their ends.
Inputs may be any that keep to these rules, and one draw needn't show every extreme that they name: `first_picks`: each token names 6 different experts. `second_picks`: each token names 6 different experts.
All inputs are finite; a program needn't handle non-finite values.
Results may differ from the reference program's by a relative error of at most 0.002.
The reference program's roundings to bfloat16 on the way (of `normed` and `hidden`) count: a program that leaves them out, or rounds other values in their place, can miss the bound.
Values may be sent and summed in bfloat16 or wider, within the bound.
No kernel may reach another device: no remote copies, remote signals or barrier semaphores. Data moves between devices by JAX's collectives and lax.ppermute only.
A program may use at most 64 MiB of HBM per device.

```python
import jax
import jax.numpy as jnp
from jax import lax

D = 2048
F = 1280
E = 64
TOP = 6
SEQ = 512
SEQS = 2
SECTIONS = 4


def draw_first_input(key, part):
    common = jax.random.normal(jax.random.fold_in(key, 7), (SECTIONS, 1, 1, D), jnp.float32)
    noise = jax.random.normal(jax.random.fold_in(key, 13), (SECTIONS, SEQS, SEQ, D), jnp.float32)
    values = noise + 1.5 * common
    return jnp.clip(values, -14.0, 14.0).astype(jnp.bfloat16)


def levels(stream_key, shape, cuts, smallest, high):
    loudness, own = 1.0, jax.random.fold_in(stream_key, 6)
    for axis_at, blocks in cuts:
        draws = jnp.exp(jax.random.uniform(jax.random.fold_in(own, axis_at), (blocks,), jnp.float32, smallest / len(cuts), high / len(cuts)))
        loudness = loudness * jnp.repeat(draws, shape[axis_at] // blocks).reshape([-1 if axis == axis_at else 1 for axis in range(len(shape))])
    return loudness


def distinct(own_key, rows, amount, top, lift):
    sequence = jax.random.permutation(jax.random.fold_in(own_key, 1), amount)
    favour = sequence
    for power in range(3):
        favour = favour * favour // amount
    favour = favour * lift // amount
    chance = jax.random.randint(jax.random.fold_in(own_key, 2), (rows, amount), 0, 4096) + favour
    sure = jax.random.permutation(jax.random.fold_in(own_key, 3), rows)[jnp.arange(amount) % rows]
    chance = jnp.where(jnp.arange(rows)[:, None] == sure[None, :], 1 << 14, chance)
    priority = chance * amount + jnp.arange(amount)
    return lax.top_k(priority.astype(jnp.int32), top)[1].astype(jnp.int32)


def bell_draw(rng, extent, width, limit, cuts=(), kind=jnp.bfloat16):
    values = jax.random.normal(rng, extent, jnp.float32) * width
    if len(cuts) > 0:
        values = levels(rng, extent, cuts, -0.22, 0.18) * values
    return jnp.clip(values, min=-limit, max=limit).astype(kind)


def setup_inputs(seed: int = 0) -> dict:
    keys = jax.random.split(jax.random.key(seed), 12)
    first_input = draw_first_input(jax.random.fold_in(keys[11], 71), 0)
    second_input = bell_draw(keys[1], (SECTIONS, SEQS, SEQ, D), 1.0, 6.0, ((0, 4), (1, 2), (2, 4)))
    upstream = bell_draw(keys[2], (SECTIONS, SEQS, SEQ, D), 1.0, 6.0, ((0, 4), (1, 2), (2, 4)))
    first_picks = distinct(keys[3], SECTIONS * SEQS * SEQ, E, TOP, 768).reshape((SECTIONS, SEQS, SEQ, TOP))
    second_picks = distinct(keys[4], SECTIONS * SEQS * SEQ, E, TOP, 768).reshape((SECTIONS, SEQS, SEQ, TOP))
    gate_grads = bell_draw(keys[5], (SECTIONS, SEQS, SEQ, TOP), 0.00015, 0.0009, ((0, 4), (1, 2), (2, 4)), jnp.float32)
    norm_gain = jnp.clip(1.0 + 0.1 * jax.random.normal(keys[6], (SECTIONS, D), jnp.float32), 0.5, 1.5)
    router_weight = bell_draw(keys[7], (SECTIONS, E, D), (D // 4) ** -0.5, 0.25, ((0, 4),), jnp.float32)
    gate_weight = bell_draw(keys[8], (SECTIONS, D, F), D ** -0.5, 0.125, ((0, 4), (1, 4)))
    up_weight = bell_draw(keys[9], (SECTIONS, D, F), D ** -0.5, 0.125, ((0, 4), (1, 4)))
    down_weight = bell_draw(keys[10], (SECTIONS, F, D), F ** -0.5, 0.15625, ((0, 4), (2, 4)))
    return {"first_input": first_input, "second_input": second_input, "upstream": upstream, "first_picks": first_picks, "second_picks": second_picks, "gate_grads": gate_grads, "norm_gain": norm_gain, "router_weight": router_weight, "gate_weight": gate_weight, "up_weight": up_weight, "down_weight": down_weight}


EPSILON = 1e-06
ROUTE_SCALE = 2.5

def normalize(values_in, norm_gain):
    values = values_in.astype(jnp.float32)
    inverse = lax.rsqrt(lax.optimization_barrier(jnp.mean(values * values, axis=-1, keepdims=True)) + EPSILON)
    return ((values * inverse * norm_gain).astype(jnp.bfloat16), inverse)

def one_hot(picks, experts):
    labels = jnp.arange(experts, dtype=jnp.int32)
    return (picks[:, :, None] == labels[None, None, :]).astype(jnp.float32)

def scores(normed, router_w, table):
    logits = jnp.dot(normed.astype(jnp.float32), router_w.T, precision=lax.Precision.HIGHEST)
    affinity = jax.nn.sigmoid(logits)
    chosen = jnp.einsum('tke,te->tk', table, affinity, precision=lax.Precision.HIGHEST)
    chosen_sum = lax.optimization_barrier(jnp.sum(chosen, axis=-1, keepdims=True))
    gate_weights = ROUTE_SCALE * chosen / chosen_sum
    spread = lax.optimization_barrier(jnp.sum(affinity, axis=-1, keepdims=True))
    shares = affinity / spread
    return (affinity, chosen, chosen_sum, gate_weights, spread, shares)

def router_back(grads, table, affinity, chosen, chosen_sum, spread, shares, frac, length):
    chosen_grad = ROUTE_SCALE * (grads / chosen_sum - lax.optimization_barrier(jnp.sum(grads * chosen, axis=-1, keepdims=True)) / (chosen_sum * chosen_sum))
    affinity_grad = jnp.einsum('tk,tke->te', chosen_grad, table, precision=lax.Precision.HIGHEST)
    share_grad = frac[None, :] / length
    affinity_grad = affinity_grad + (share_grad - lax.optimization_barrier(jnp.sum(share_grad * shares, axis=-1, keepdims=True))) / spread
    return affinity_grad * affinity * (1.0 - affinity)

def shared_back(hidden_grad, gate_pre, up_pre):
    sigmoid_v = jax.nn.sigmoid(gate_pre)
    slope = sigmoid_v * (1.0 + gate_pre * (1.0 - sigmoid_v))
    gate_grad = (hidden_grad * up_pre * slope).astype(jnp.bfloat16)
    up_grad = (hidden_grad * gate_pre * sigmoid_v).astype(jnp.bfloat16)
    return (gate_grad, up_grad)

def norm_back(values_in, inverse, norm_gain, normed_grad):
    values = values_in.astype(jnp.float32)
    scaled = normed_grad * norm_gain
    return inverse * (scaled - values * inverse * inverse * lax.optimization_barrier(jnp.mean(scaled * values, axis=-1, keepdims=True)))

def window(first_in, second_in, returned, first_pk, second_pk, grads, norm_gain, router_w, gate_w, up_w, down_w):
    length = first_in.shape[0]
    experts = router_w.shape[0]
    per_token = first_pk.shape[1]
    normed_a, inverse_a = normalize(first_in, norm_gain)
    normed_b, inverse_b = normalize(second_in, norm_gain)
    table_a = one_hot(first_pk, experts)
    table_b = one_hot(second_pk, experts)
    aff_a, chosen_a, csum_a, routing_a, spread_a, shares_a = scores(normed_a, router_w, table_a)
    aff_b, chosen_b, csum_b, routing_b, spread_b, shares_b = scores(normed_b, router_w, table_b)
    frac_a = experts / (per_token * length) * lax.optimization_barrier(jnp.sum(table_a, axis=(0, 1)))
    frac_b = experts / (per_token * length) * lax.optimization_barrier(jnp.sum(table_b, axis=(0, 1)))
    balance = jnp.stack([jnp.sum(frac_a * lax.optimization_barrier(jnp.sum(shares_a, axis=0)) / length), jnp.sum(frac_b * lax.optimization_barrier(jnp.sum(shares_b, axis=0)) / length)])
    stacked = jnp.concatenate([normed_a, normed_b], axis=0)
    gate_pre = jnp.dot(stacked, gate_w, preferred_element_type=jnp.float32)
    up_pre = jnp.dot(stacked, up_w, preferred_element_type=jnp.float32)
    hidden = (jax.nn.silu(gate_pre) * up_pre).astype(jnp.bfloat16)
    output_a = (first_in.astype(jnp.float32) + jnp.dot(hidden[:length], down_w, preferred_element_type=jnp.float32)).astype(jnp.bfloat16)
    hidden_grad = jnp.dot(returned, down_w.T, preferred_element_type=jnp.float32)
    gate_grad, up_grad = shared_back(hidden_grad, gate_pre[length:], up_pre[length:])
    normed_grad = jnp.dot(gate_grad, gate_w.T, preferred_element_type=jnp.float32) + jnp.dot(up_grad, up_w.T, preferred_element_type=jnp.float32)
    logit_grad = router_back(grads, table_b, aff_b, chosen_b, csum_b, spread_b, shares_b, frac_b, length)
    router_part = jnp.dot(logit_grad.T, normed_b.astype(jnp.float32), precision=lax.Precision.HIGHEST)
    normed_grad = normed_grad + jnp.dot(logit_grad, router_w, precision=lax.Precision.HIGHEST)
    input_grad = (returned.astype(jnp.float32) + norm_back(second_in, inverse_b, norm_gain, normed_grad)).astype(jnp.bfloat16)
    return (output_a, routing_a, input_grad, router_part, balance)

def reference(first_input, second_input, upstream, first_picks, second_picks, gate_grads, norm_gain, router_weight, gate_weight, up_weight, down_weight):
    returned_all = jnp.roll(upstream, -1, axis=0)

    def per_section(section_args):
        first_in, second_in, returned, first_pk, second_pk, grads, gain_s, router_s, gate_s, up_s, down_s = section_args

        def per_seq(seq_args):
            return window(*seq_args, gain_s, router_s, gate_s, up_s, down_s)
        return lax.map(per_seq, (first_in, second_in, returned, first_pk, second_pk, grads))
    outputs, routing, input_grad, router_parts, balance = lax.map(per_section, (first_input, second_input, returned_all, first_picks, second_picks, gate_grads, norm_gain, router_weight, gate_weight, up_weight, down_weight))
    arrived = jnp.roll(outputs, 1, axis=0)
    return (arrived, routing, input_grad, lax.optimization_barrier(jnp.sum(router_parts, axis=1)), balance)
```

```python
import jax
import jax.numpy as jnp
from jax import lax
from jax.sharding import PartitionSpec as P

EPSILON = 1e-06
ROUTE_SCALE = 2.5


def shifted(block, axis, distance):
    devices = range(lax.axis_size(axis))
    route = [((i - distance) % len(devices), i) for i in devices]
    return lax.ppermute(block, axis, route)


def siblings(axis):
    size = lax.axis_size(axis)
    return [(i, i ^ 1) for i in range(size)]


def gather_split(block, axis, shard_axis):
    if lax.axis_size("dp") % 2:
        return lax.all_gather(block, axis, axis=shard_axis, tiled=True)
    core = lax.axis_index("dp") % 2
    rows = block.shape[0] // 2
    mine = lax.dynamic_slice_in_dim(block, core * rows, rows, axis=0)
    mine = lax.all_gather(mine, axis, axis=0, tiled=False)
    other = lax.ppermute(mine, "dp", siblings("dp"))
    both = jnp.stack([jnp.where(core == 0, mine, other), jnp.where(core == 0, other, mine)], axis=1)
    if shard_axis == 0:
        return both.reshape(-1, block.shape[1])
    return both.reshape(-1, block.shape[0], block.shape[1]).transpose(1, 0, 2).reshape(block.shape[0], -1)


def normalize(values_in, norm_gain):
    values = values_in.astype(jnp.float32)
    inverse = lax.rsqrt(jnp.mean(values * values, axis=-1, keepdims=True) + EPSILON)
    return ((values * inverse * norm_gain).astype(jnp.bfloat16), inverse)


def one_hot(picks, experts):
    labels = jnp.arange(experts, dtype=jnp.int32)
    return (picks[:, :, None] == labels[None, None, :]).astype(jnp.float32)


def scores(normed, router_w, table):
    logits = jnp.dot(normed.astype(jnp.float32), router_w.T, precision=lax.Precision.HIGHEST)
    affinity = jax.nn.sigmoid(logits)
    chosen = jnp.einsum("tke,te->tk", table, affinity, precision=lax.Precision.HIGHEST)
    chosen_sum = jnp.sum(chosen, axis=-1, keepdims=True)
    gate_weights = ROUTE_SCALE * chosen / chosen_sum
    spread = jnp.sum(affinity, axis=-1, keepdims=True)
    shares = affinity / spread
    return (affinity, chosen, chosen_sum, gate_weights, spread, shares)


def router_back(grads, table, affinity, chosen, chosen_sum, spread, shares, frac, length):
    chosen_grad = ROUTE_SCALE * (
        grads / chosen_sum
        - jnp.sum(grads * chosen, axis=-1, keepdims=True) / (chosen_sum * chosen_sum)
    )
    affinity_grad = jnp.einsum("tk,tke->te", chosen_grad, table, precision=lax.Precision.HIGHEST)
    share_grad = frac[None, :] / length
    affinity_grad = (
        affinity_grad + (share_grad - jnp.sum(share_grad * shares, axis=-1, keepdims=True)) / spread
    )
    return affinity_grad * affinity * (1.0 - affinity)


def shared_back(hidden_grad, gate_pre, up_pre):
    sigmoid_v = jax.nn.sigmoid(gate_pre)
    slope = sigmoid_v * (1.0 + gate_pre * (1.0 - sigmoid_v))
    gate_grad = (hidden_grad * up_pre * slope).astype(jnp.bfloat16)
    up_grad = (hidden_grad * gate_pre * sigmoid_v).astype(jnp.bfloat16)
    return (gate_grad, up_grad)


def norm_back(values_in, inverse, norm_gain, normed_grad):
    values = values_in.astype(jnp.float32)
    scaled = normed_grad * norm_gain
    return inverse * (
        scaled - values * inverse * inverse * jnp.mean(scaled * values, axis=-1, keepdims=True)
    )


def shards(
    first_input,
    second_input,
    upstream,
    first_picks,
    second_picks,
    gate_grads,
    norm_gain,
    router_weight,
    gate_weight,
    up_weight,
    down_weight,
):
    first_in = first_input[0, 0]
    second_in = second_input[0, 0]
    first_pk = first_picks[0, 0]
    second_pk = second_picks[0, 0]
    grads = gate_grads[0, 0]
    gain_s = norm_gain[0]
    router_w = router_weight[0]
    experts = router_w.shape[0]
    tokens = first_in.shape[0]
    per_token = first_pk.shape[1]
    length = tokens * lax.axis_size("ctx")
    table_a = one_hot(first_pk, experts)
    table_b = one_hot(second_pk, experts)
    counts_a = jnp.sum(table_a, axis=(0, 1))
    counts_b = jnp.sum(table_b, axis=(0, 1))
    returned = shifted(upstream[0, 0], "section", -1)
    normed_a, inverse_a = normalize(first_in, gain_s)
    normed_b, inverse_b = normalize(second_in, gain_s)
    aff_a, chosen_a, csum_a, routing_a, spread_a, shares_a = scores(normed_a, router_w, table_a)
    aff_b, chosen_b, csum_b, routing_b, spread_b, shares_b = scores(normed_b, router_w, table_b)
    sums_a = jnp.sum(shares_a, axis=0)
    sums_b = jnp.sum(shares_b, axis=0)
    counts_a, counts_b, sums_a, sums_b = lax.psum((counts_a, counts_b, sums_a, sums_b), "ctx")
    frac_a = experts / (per_token * length) * counts_a
    frac_b = experts / (per_token * length) * counts_b
    balance = jnp.stack([jnp.sum(frac_a * sums_a / length), jnp.sum(frac_b * sums_b / length)])
    stacked = jnp.concatenate([normed_a, normed_b], axis=0)
    gate_full, up_full, down_full = (
        gather_split(gate_weight[0], "ctx", 0),
        gather_split(up_weight[0], "ctx", 0),
        gather_split(down_weight[0], "ctx", 1),
    )
    gate_pre = jnp.dot(stacked, gate_full, preferred_element_type=jnp.float32)
    up_pre = jnp.dot(stacked, up_full, preferred_element_type=jnp.float32)
    hidden = (jax.nn.silu(gate_pre) * up_pre).astype(jnp.bfloat16)
    projected = jnp.dot(hidden[:tokens], down_full, preferred_element_type=jnp.float32)
    hidden_grad = jnp.einsum("td,fd->tf", returned, down_full, preferred_element_type=jnp.float32)
    output_a = (first_in.astype(jnp.float32) + projected).astype(jnp.bfloat16)
    arrived = shifted(output_a, "section", 1)
    gate_grad, up_grad = shared_back(hidden_grad, gate_pre[tokens:], up_pre[tokens:])
    normed_grad = jnp.einsum("tf,df->td", gate_grad, gate_full, preferred_element_type=jnp.float32)
    normed_grad = normed_grad + jnp.einsum(
        "tf,df->td", up_grad, up_full, preferred_element_type=jnp.float32
    )
    logit_grad = router_back(
        grads, table_b, aff_b, chosen_b, csum_b, spread_b, shares_b, frac_b, length
    )
    router_part = jnp.dot(
        logit_grad.T, normed_b.astype(jnp.float32), precision=lax.Precision.HIGHEST
    )
    normed_grad = normed_grad + jnp.dot(logit_grad, router_w, precision=lax.Precision.HIGHEST)
    input_grad = (
        returned.astype(jnp.float32) + norm_back(second_in, inverse_b, gain_s, normed_grad)
    ).astype(jnp.bfloat16)
    router_total = lax.psum(router_part, ("ctx", "dp"))
    return (
        arrived[None, None],
        routing_a[None, None],
        input_grad[None, None],
        router_total[None],
        balance[None, None],
    )


def solution(mesh):
    in_specs = (
        P("section", "dp", "ctx", None),
        P("section", "dp", "ctx", None),
        P("section", "dp", "ctx", None),
        P("section", "dp", "ctx", None),
        P("section", "dp", "ctx", None),
        P("section", "dp", "ctx", None),
        P("section", None),
        P("section", None, None),
        P("section", "ctx", None),
        P("section", "ctx", None),
        P("section", None, "ctx"),
    )
    out_specs = (
        P("section", "dp", "ctx", None),
        P("section", "dp", "ctx", None),
        P("section", "dp", "ctx", None),
        P("section", None, None),
        P("section", "dp", None),
    )
    return jax.shard_map(shards, mesh=mesh, in_specs=in_specs, out_specs=out_specs, check_vma=False)
```
